768 devices in a mesh: gx: 12 (over z), gy: 8 (over y_lo, x), gz: 8 (over y_hi, core).
Axes of the slice: x: 4, y: 8 (y_hi: 4, y_lo: 2; y = y_hi * 2 + y_lo), z: 12, core: 2. Of those that a mesh axis runs over, the one named last changes fastest.
Arguments:
- metric: float32 [6, 192, 128, 1024], P(None, 'gx', 'gy', 'gz'), may hold values from -1 to 9
- curvature: float32 [6, 192, 128, 1024], P(None, 'gx', 'gy', 'gz'), may hold values from -1.8 to 1.8
- conserved: float32 [4, 192, 128, 1024], P(None, 'gx', 'gy', 'gz'), may hold values from -0.3 to 1, as said below
- matter_mask: int32 [12, 8, 64], P('gx', 'gy', 'gz'), may hold values from 0 to 1, as said below
Outputs:
- metric_next: float32 [6, 192, 128, 1024], P(None, 'gx', 'gy', 'gz')
- curvature_next: float32 [6, 192, 128, 1024], P(None, 'gx', 'gy', 'gz')
- conserved_next: float32 [4, 192, 128, 1024], P(None, 'gx', 'gy', 'gz')
The draws below stay inside these ranges and needn't reach their ends.
Inputs may be any that keep to these rules, and one draw needn't show every extreme that they name: `conserved`: component 0 is the density, from 0.25 to 1; components 1 to 3 are the momentum. `matter_mask`: 1 marks a matter-bearing meshblock of 16 x 16 x 16 cells.
All inputs are finite; a program needn't handle non-finite values.
Results may differ from the reference program's by a relative error of at most 0.00002.
Values sent between devices are 32-bit elements; how exact they have to be, the bound alone decides.
A program may use at most 32 MiB of HBM per device.

```python
import math
import jax
import jax.numpy as jnp

MB = 16
NX = 192
NY = 128
NZ = 1024
KX = 12
KY = 8
KZ = 64


def draw_metric(key, part):
    key_phase = jax.random.fold_in(key, 31)
    key_rough = jax.random.fold_in(key, 32)
    phases = jax.random.uniform(key_phase, (6, 3), jnp.float32, 0.0, 2.0 * jnp.pi)
    coord_x = 2.0 * jnp.pi / NX * jnp.arange(NX, dtype=jnp.float32)
    coord_y = 2.0 * jnp.pi / NY * jnp.arange(NY, dtype=jnp.float32)
    coord_z = 2.0 * jnp.pi / NZ * jnp.arange(NZ, dtype=jnp.float32)
    wave_x = jnp.cos(coord_x[None, :] + phases[:, 0:1])[:, :, None, None]
    wave_y = jnp.cos(coord_y[None, :] + phases[:, 1:2])[:, None, :, None]
    wave_z = jnp.cos(coord_z[None, :] + phases[:, 2:3])[:, None, None, :]
    smooth = 1.5 * wave_x * wave_y * wave_z
    rough = jnp.clip(jax.random.normal(key_rough, (6, NX, NY, NZ), jnp.float32), -3.0, 3.0)
    return 4.0 + smooth + rough


def draw_conserved(key, part):
    key_density = jax.random.fold_in(key, 11)
    key_moment = jax.random.fold_in(key, 12)
    position = jnp.arange(NX, dtype=jnp.float32) / max(NX - 1, 1)
    density = jnp.exp(jax.random.uniform(key_density, (1, NX, NY, NZ), jnp.float32, jnp.log(0.25), jnp.log(1.0)))
    rising = (0.03 * (1.0 + 2.0 * position))[None, :, None, None]
    moment = jnp.clip(jax.random.normal(key_moment, (3, NX, NY, NZ), jnp.float32), -3.0, 3.0) * rising
    return jnp.concatenate([density, moment], axis=0)


def draw_matter_mask(key, part):
    index_x = jnp.arange(KX, dtype=jnp.int32)[:, None, None]
    index_y = jnp.arange(KY, dtype=jnp.int32)[None, :, None]
    index_z = jnp.arange(KZ, dtype=jnp.int32)[None, None, :]
    offset_x = 2 * index_x + 1 - KX
    offset_y = 2 * index_y + 1 - KY
    offset_z = 2 * index_z + 1 - KZ
    radius = offset_x * offset_x * 100 // (KX * KX) + offset_y * offset_y * 100 // (KY * KY) + offset_z * offset_z * 100 // (KZ * KZ)
    threshold = jnp.maximum(700 - 5 * radius, 30)
    sample = jax.random.randint(jax.random.fold_in(key, 21), (KX, KY, KZ), 0, 1000)
    return (sample < threshold).astype(jnp.int32)


def shard_levels(stream_key, shape, cuts, smallest, top_value):
    factor_of = 1.0
    for dim, parts in cuts:
        draws = jax.random.uniform(jax.random.fold_in(jax.random.fold_in(stream_key, 6), dim), (parts,), jnp.float32, smallest / len(cuts), top_value / len(cuts))
        factor_of = factor_of * jnp.repeat(jnp.exp(draws), shape[dim] // parts).reshape((-1,) + (1,) * (len(shape) - 1 - dim))
    return factor_of


def bell_draw(stream_key, extent, deviation, bound, split=(), held_as=jnp.bfloat16):
    array = deviation * jax.random.normal(stream_key, extent, jnp.float32)
    if split:
        array = array * shard_levels(stream_key, extent, split, -0.22, 0.18)
    return jnp.clip(array, -bound, bound).astype(held_as)


def setup_inputs(seed: int = 0) -> dict:
    arg_keys = jax.random.split(jax.random.key(seed), 5)
    metric = draw_metric(jax.random.fold_in(arg_keys[4], 71), 0)
    curvature = bell_draw(arg_keys[1], (6, NX, NY, NZ), 0.3, 1.8, ((1, 12), (2, 8), (3, 8)), jnp.float32)
    conserved = draw_conserved(jax.random.fold_in(arg_keys[4], 71), 0)
    matter_mask = draw_matter_mask(jax.random.fold_in(arg_keys[4], 71), 0)
    return dict(metric=metric, curvature=curvature, conserved=conserved, matter_mask=matter_mask)


second_stencil = (1.0 / 90.0, -3.0 / 20.0, 1.5, -49.0 / 18.0, 1.5, -3.0 / 20.0, 1.0 / 90.0)
first_stencil = (-1.0 / 60.0, 3.0 / 20.0, -0.75, 0.0, 0.75, -3.0 / 20.0, 1.0 / 60.0)
sound_square = 0.25
sound_speed = 0.5
courant = 0.3
eight_pi = 8.0 * math.pi
pair_first = (0, 0, 0, 1, 1, 2)
pair_second = (0, 1, 2, 1, 2, 2)


def expand_mask(matter_mask, block_edge):
    blocks_x, blocks_y, blocks_z = matter_mask.shape
    spread = jnp.broadcast_to(matter_mask[:, None, :, None, :, None], (blocks_x, block_edge, blocks_y, block_edge, blocks_z, block_edge))
    return spread.reshape(blocks_x * block_edge, blocks_y * block_edge, blocks_z * block_edge) > 0


def rolled_sum(field, stencil, axis_index):
    total = jnp.zeros_like(field)
    for offset in range(-3, 4):
        if stencil[offset + 3] != 0.0:
            total = total + stencil[offset + 3] * jnp.roll(field, -offset, axis=axis_index)
    return total


def reference(metric, curvature, conserved, matter_mask):
    cell_mask = expand_mask(matter_mask, MB)
    density = conserved[0]
    moment = conserved[1:4]
    speed = jnp.max(jnp.abs(moment), axis=0) / density + sound_speed
    speed_max = jnp.max(jnp.where(cell_mask, speed, jnp.float32(sound_speed)))
    step = courant / speed_max
    laplacian = rolled_sum(metric, second_stencil, 1)
    laplacian = laplacian + rolled_sum(metric, second_stencil, 2)
    laplacian = laplacian + rolled_sum(metric, second_stencil, 3)
    stress_list = []
    for component in range(6):
        first = pair_first[component]
        second = pair_second[component]
        term = moment[first] * moment[second] / density
        if first == second:
            term = term + sound_square * density
        stress_list.append(term)
    stress = jnp.stack(stress_list)
    curvature_next = curvature + step * (eight_pi * stress - 0.5 * laplacian)
    metric_next = metric - 2.0 * step * curvature
    potential = 0.5 * (metric[0] + metric[3] + metric[5])
    gradient = jnp.stack([rolled_sum(potential, first_stencil, direction) for direction in range(3)])
    divergence = jnp.zeros_like(conserved)
    for direction in range(3):
        velocity = moment[direction] / density
        flux_moment = moment * velocity[None]
        flux_moment = flux_moment.at[direction].add(sound_square * density)
        flux = jnp.concatenate([moment[direction][None], flux_moment], axis=0)
        upper_flux = jnp.roll(flux, -1, axis=direction + 1)
        upper_state = jnp.roll(conserved, -1, axis=direction + 1)
        face = 0.5 * (flux + upper_flux) - 0.5 * speed_max * (upper_state - conserved)
        divergence = divergence + (face - jnp.roll(face, 1, axis=direction + 1))
    source = jnp.concatenate([jnp.zeros_like(density)[None], density[None] * gradient], axis=0)
    advanced = conserved - step * divergence + step * source
    conserved_next = jnp.where(cell_mask[None], advanced, conserved)
    return metric_next, curvature_next, conserved_next
```

```python
import math

import jax
import jax.numpy as jnp
from jax import lax
from jax.experimental import pallas as pl
from jax.experimental.pallas import tpu as pltpu
from jax.sharding import PartitionSpec as P

MESH = pl.DeviceIdType.MESH
MB = 16
second_stencil = (1.0 / 90.0, -3.0 / 20.0, 1.5, -49.0 / 18.0)
first_stencil = (-1.0 / 60.0, 3.0 / 20.0, -0.75)
sound_square = 0.25
sound_speed = 0.5
courant = 0.3
eight_pi = 8.0 * math.pi
pair_first = (0, 0, 0, 1, 1, 2)
pair_second = (0, 1, 2, 1, 2, 2)
diagonal = (0, 3, 5)

X, Y_LO, Y_HI, CORES = 4, 2, 4, 2
Y = Y_LO * Y_HI


def kernel(
    gx_size,
    metric_hbm, curvature_hbm, conserved_hbm, mask_hbm,
    plain, curv, rhs, held, slope, step_out,
    met, flu, inv, mask,
    pack_up, pack_down, from_low, from_high,
    own, got_1, got_2, got_3,
    local_sem, halo_send, halo_recv, max_send, max_recv,
):
    gx, gy, gz = lax.axis_index("gx"), lax.axis_index("gy"), lax.axis_index("gz")
    x, y_lo = lax.rem(gy, X), gy // X
    core, y_hi = lax.rem(gz, CORES), gz // CORES
    y = y_hi * Y_LO + y_lo
    gy_size, gz_size = X * Y_LO, Y_HI * CORES

    load_flu = pltpu.make_async_copy(conserved_hbm, flu.at[:, 1:17, 8:24, :], local_sem.at[0])
    load_mask = pltpu.make_async_copy(mask_hbm, mask, local_sem.at[1])
    load_met = pltpu.make_async_copy(metric_hbm, met.at[:, 3:19, 8:24, :], local_sem.at[2])
    load_curv = pltpu.make_async_copy(curvature_hbm, curv, local_sem.at[3])
    load_flu.start()
    load_mask.start()
    load_met.start()
    load_curv.start()
    load_plain = pltpu.make_async_copy(metric_hbm, plain, local_sem.at[4])
    load_plain.start()

    group_1 = []
    for dx in range(X):
        for dc in range(CORES):
            if dx or dc:
                group_1.append(
                    {"gx": gx, "gy": y_lo * X + lax.rem(x + dx, X), "gz": y_hi * CORES + lax.rem(core + dc, CORES)}
                )
    group_2 = []
    for dy in range(1, Y):
        there = lax.rem(y + dy, Y)
        group_2.append({"gx": gx, "gy": lax.rem(there, Y_LO) * X + x, "gz": (there // Y_LO) * CORES + core})
    group_3 = [{"gx": lax.rem(gx + dz, gx_size), "gy": gy, "gz": gz} for dz in range(1, gx_size)]
    x_up = {"gx": lax.rem(gx + 1, gx_size), "gy": gy, "gz": gz}
    x_down = {"gx": lax.rem(gx + gx_size - 1, gx_size), "gy": gy, "gz": gz}
    y_up = {"gx": gx, "gy": lax.rem(gy + 1, gy_size), "gz": gz}
    y_down = {"gx": gx, "gy": lax.rem(gy + gy_size - 1, gy_size), "gz": gz}
    z_up = {"gx": gx, "gy": gy, "gz": lax.rem(gz + 1, gz_size)}
    z_down = {"gx": gx, "gy": gy, "gz": lax.rem(gz + gz_size - 1, gz_size)}

    barrier = pltpu.get_barrier_semaphore()
    greeted = group_1 + group_2 + group_3 + [y_up, y_down, z_up, z_down]
    for peer in greeted:
        pl.semaphore_signal(barrier, inc=1, device_id=peer, device_id_type=MESH)

    load_flu.wait()
    load_mask.wait()
    lane = lax.broadcasted_iota(jnp.int32, (16, 128), 1)
    block = lane // MB
    matter = jnp.zeros((16, 128), jnp.int32)
    for b in range(128 // MB):
        matter = jnp.where(block == b, mask[0, 0, b], matter)
    live = matter > 0
    fastest = jnp.full((16, 128), sound_speed, jnp.float32)
    for i in range(16):
        density = flu[0, 1 + i, 8:24, :]
        largest = jnp.abs(flu[1, 1 + i, 8:24, :])
        for d in (2, 3):
            largest = jnp.maximum(largest, jnp.abs(flu[d, 1 + i, 8:24, :]))
        fastest = jnp.maximum(fastest, jnp.where(live, largest / density + sound_speed, sound_speed))
    own[0] = jnp.max(fastest, axis=0, keepdims=True)

    pl.semaphore_wait(barrier, len(greeted))

    sends = []

    def spread(stage, group, got, first):
        copies = []
        for slot, peer in enumerate(group):
            copy = pltpu.make_async_remote_copy(
                src_ref=own.at[stage],
                dst_ref=got.at[slot],
                send_sem=max_send.at[first + slot],
                recv_sem=max_recv.at[first + slot],
                device_id=peer,
                device_id_type=MESH,
            )
            copy.start()
            copies.append(copy)
        sends.extend(copies)
        return copies

    def gather(copies, stage, got):
        for copy in copies:
            copy.wait_recv()
        best = own[stage]
        for slot in range(len(copies)):
            best = jnp.maximum(best, got[slot])
        return best

    stage_1 = spread(0, group_1, got_1, 0)

    halos = []

    def send_halo(src, dst, peer):
        n = len(halos)
        copy = pltpu.make_async_remote_copy(
            src_ref=src,
            dst_ref=dst,
            send_sem=halo_send.at[n],
            recv_sem=halo_recv.at[n],
            device_id=peer,
            device_id_type=MESH,
        )
        copy.start()
        halos.append(copy)

    send_halo(flu.at[:, 16:17, 8:24, :], flu.at[:, 0:1, 8:24, :], x_up)
    send_halo(flu.at[:, 1:2, 8:24, :], flu.at[:, 17:18, 8:24, :], x_down)
    send_halo(flu.at[:, 1:17, 23:24, :], flu.at[:, 1:17, 7:8, :], y_up)
    send_halo(flu.at[:, 1:17, 8:9, :], flu.at[:, 1:17, 24:25, :], y_down)
    load_met.wait()
    send_halo(met.at[:, 16:19, 8:24, :], met.at[:, 0:3, 8:24, :], x_up)
    send_halo(met.at[:, 3:6, 8:24, :], met.at[:, 19:22, 8:24, :], x_down)
    send_halo(met.at[:, 3:19, 21:24, :], met.at[:, 3:19, 5:8, :], y_up)
    send_halo(met.at[:, 3:19, 8:11, :], met.at[:, 3:19, 24:27, :], y_down)

    group_of = lane // 4
    for f in range(5):
        up = jnp.zeros((16, 128), jnp.float32)
        down = jnp.zeros((16, 128), jnp.float32)
        for half in range(2):
            c = 2 * f + half
            for i in range(16):
                k = half * 16 + i
                plane = met[c, 3 + i, 8:24, :] if c < 6 else flu[c - 6, 1 + i, 8:24, :]
                up = jnp.where(group_of == k, pltpu.roll(plane, (4 * k + 4) % 128, 1), up)
                down = jnp.where(group_of == k, pltpu.roll(plane, 4 * k, 1) if k else plane, down)
        pack_up[f] = up
        pack_down[f] = down
    send_halo(pack_up, from_low, z_up)
    send_halo(pack_down, from_high, z_down)

    own[1] = gather(stage_1, 0, got_1)
    stage_2 = spread(1, group_2, got_2, len(group_1))
    own[2] = gather(stage_2, 1, got_2)
    stage_3 = spread(2, group_3, got_3, len(group_1) + len(group_2))

    for copy in halos:
        copy.wait_recv()
    load_curv.wait()
    load_plain.wait()

    for i in range(18):
        inv[i] = 1.0 / flu[0, i]

    def plane_step(i, carry):
        def z_halo(c):
            k = (c % 2) * 16 + i
            low = pltpu.roll(from_low[c // 2], lax.rem(124 - 4 * k + 128, 128), 1)
            high = pltpu.roll(from_high[c // 2], lax.rem(128 - 4 * k, 128), 1)
            return low, high

        def along_z(value, low, high, offset):
            if offset > 0:
                return pltpu.roll(jnp.where(lane < offset, high, value), 128 - offset, 1)
            return pltpu.roll(jnp.where(lane >= 128 + offset, low, value), -offset, 1)

        density = flu[0, 1 + i, 8:24, :]
        inverse = inv[1 + i, 8:24, :]
        moment = [flu[1 + d, 1 + i, 8:24, :] for d in range(3)]
        velocity = [m * inverse for m in moment]

        potential = {}
        for c in range(6):
            low, high = z_halo(c)
            value = met[c, 3 + i, 8:24, :]
            laplacian = (3.0 * second_stencil[3]) * value
            for n in range(3):
                o = 3 - n
                pairs = (
                    (met[c, 3 + i + o, 8:24, :], met[c, 3 + i - o, 8:24, :]),
                    (met[c, 3 + i, 8 + o : 24 + o, :], met[c, 3 + i, 8 - o : 24 - o, :]),
                    (along_z(value, low, high, o), along_z(value, low, high, -o)),
                )
                total = None
                for d, (above, below) in enumerate(pairs):
                    both = above + below
                    total = both if total is None else total + both
                    if c in diagonal:
                        change = above - below
                        key = (d, n)
                        potential[key] = change if key not in potential else potential[key] + change
                laplacian = laplacian + second_stencil[n] * total
            a, b = pair_first[c], pair_second[c]
            stress = moment[a] * velocity[b]
            if a == b:
                stress = stress + sound_square * density
            rhs[c, i] = eight_pi * stress - 0.5 * laplacian

        def cell(dim, offset):
            if dim == 0:
                state = [flu[c, 1 + i + offset, 8:24, :] for c in range(4)]
                inverse_there = inv[1 + i + offset, 8:24, :]
            elif dim == 1:
                state = [flu[c, 1 + i, 8 + offset : 24 + offset, :] for c in range(4)]
                inverse_there = inv[1 + i, 8 + offset : 24 + offset, :]
            else:
                state = []
                for c in range(4):
                    low, high = z_halo(6 + c)
                    here = density if c == 0 else moment[c - 1]
                    state.append(along_z(here, low, high, offset))
                inverse_there = 1.0 / state[0]
            speed_there = state[1 + dim] * inverse_there
            flux = [state[1 + dim]]
            for d in range(3):
                term = state[1 + d] * speed_there
                if d == dim:
                    term = term + sound_square * state[0]
                flux.append(term)
            return state, flux

        around = [None] * 4
        outflow = [None] * 4
        for dim in range(3):
            state_up, flux_up = cell(dim, 1)
            state_down, flux_down = cell(dim, -1)
            for c in range(4):
                both = state_up[c] + state_down[c]
                net = flux_up[c] - flux_down[c]
                around[c] = both if around[c] is None else around[c] + both
                outflow[c] = net if outflow[c] is None else outflow[c] + net
        here = [density] + moment
        for c in range(4):
            kept = here[c] + (0.5 * courant) * (around[c] - 6.0 * here[c])
            rate = -0.5 * outflow[c]
            if c > 0:
                gradient = None
                for n in range(3):
                    term = (-0.5 * first_stencil[n]) * potential[(c - 1, n)]
                    gradient = term if gradient is None else gradient + term
                rate = rate + density * gradient
            held[c, i] = jnp.where(live, kept, here[c])
            slope[c, i] = jnp.where(live, rate, 0.0)
        return carry

    lax.fori_loop(0, 16, plane_step, 0)

    best = gather(stage_3, 2, got_3)
    speed_max = jnp.max(best, axis=1, keepdims=True)
    step_out[...] = jnp.broadcast_to(courant / speed_max, (16, 128))

    for copy in halos + sends:
        copy.wait_send()


def advance(plain, curv, rhs, held, slope, step_in, metric_hbm, curvature_hbm, conserved_hbm, met, bent, flu, sem):
    step = step_in[...]
    copies = []

    def put(src, dst, at):
        copy = pltpu.make_async_copy(src.at[at], dst.at[at], sem.at[len(copies)])
        copy.start()
        copies.append(copy)

    for c in range(4):
        for i in range(16):
            flu[c, i] = held[c, i] + step * slope[c, i]
        put(flu, conserved_hbm, c)
    for c in range(6):
        for i in range(16):
            bend = curv[c, i]
            met[c, i] = plain[c, i] - (2.0 * step) * bend
            bent[c, i] = bend + step * rhs[c, i]
        put(met, metric_hbm, c)
        put(bent, curvature_hbm, c)
    for copy in copies:
        copy.wait()


def body(gx_size, metric, curvature, conserved, matter_mask):
    f32 = jnp.float32
    sym, fluid = metric.shape, conserved.shape
    n_max = (X * CORES - 1) + (Y - 1) + (gx_size - 1)
    anywhere = pl.BlockSpec(memory_space=pl.ANY)
    vmem = pl.BlockSpec(memory_space=pltpu.VMEM)
    in_hbm = lambda a: pltpu.with_memory_space_constraint(a, pltpu.HBM)
    in_vmem = lambda a: pltpu.with_memory_space_constraint(a, pltpu.VMEM)
    parts = pl.pallas_call(
        lambda *refs: kernel(gx_size, *refs),
        out_shape=tuple(pltpu.VMEM(s, f32) for s in (sym, sym, sym, fluid, fluid, (16, 128))),
        in_specs=[anywhere] * 4,
        out_specs=(vmem,) * 6,
        scratch_shapes=[
            pltpu.VMEM((6, 22, 32, 128), f32),
            pltpu.VMEM((4, 18, 32, 128), f32),
            pltpu.VMEM((18, 32, 128), f32),
            pltpu.SMEM(matter_mask.shape, jnp.int32),
            pltpu.VMEM((5, 16, 128), f32),
            pltpu.VMEM((5, 16, 128), f32),
            pltpu.VMEM((5, 16, 128), f32),
            pltpu.VMEM((5, 16, 128), f32),
            pltpu.VMEM((3, 1, 128), f32),
            pltpu.VMEM((X * CORES - 1, 1, 128), f32),
            pltpu.VMEM((Y - 1, 1, 128), f32),
            pltpu.VMEM((gx_size - 1, 1, 128), f32),
            pltpu.SemaphoreType.DMA((5,)),
            pltpu.SemaphoreType.DMA((10,)),
            pltpu.SemaphoreType.DMA((10,)),
            pltpu.SemaphoreType.DMA((n_max,)),
            pltpu.SemaphoreType.DMA((n_max,)),
        ],
        compiler_params=pltpu.CompilerParams(
            collective_id=0, has_side_effects=True, vmem_limit_bytes=24 * 1024 * 1024
        ),
        name="exchange",
    )(in_hbm(metric), in_hbm(curvature), in_hbm(conserved), in_hbm(matter_mask))
    return pl.pallas_call(
        advance,
        out_shape=tuple(jax.ShapeDtypeStruct(s, f32) for s in (sym, sym, fluid)),
        in_specs=[vmem] * 6,
        out_specs=(anywhere,) * 3,
        scratch_shapes=[
            pltpu.VMEM(sym, f32),
            pltpu.VMEM(sym, f32),
            pltpu.VMEM(fluid, f32),
            pltpu.SemaphoreType.DMA((16,)),
        ],
        compiler_params=pltpu.CompilerParams(vmem_limit_bytes=16 * 1024 * 1024),
        name="advance",
    )(*(in_vmem(a) for a in parts))


def solution(mesh):
    cells = P(None, "gx", "gy", "gz")
    return jax.shard_map(
        lambda *args: body(mesh.shape["gx"], *args),
        mesh=mesh,
        in_specs=(cells, cells, cells, P("gx", "gy", "gz")),
        out_specs=(cells, cells, cells),
        check_vma=False,
    )
```

```python
import math

import jax
import jax.numpy as jnp
from jax import lax
from jax.experimental import pallas as pl
from jax.experimental.pallas import tpu as pltpu
from jax.sharding import PartitionSpec as P

MESH = pl.DeviceIdType.MESH
MB = 16
second_stencil = (1.0 / 90.0, -3.0 / 20.0, 1.5, -49.0 / 18.0)
first_stencil = (-1.0 / 60.0, 3.0 / 20.0, -0.75)
sound_square = 0.25
sound_speed = 0.5
courant = 0.3
eight_pi = 8.0 * math.pi
pair_first = (0, 0, 0, 1, 1, 2)
pair_second = (0, 1, 2, 1, 2, 2)
diagonal = (0, 3, 5)

PITCH = 40

X, Y_LO, Y_HI, CORES = 4, 2, 4, 2
Y = Y_LO * Y_HI


def far_first(n):
    return sorted(range(n), key=lambda d: -min(d, n - d))


def kernel(
    gx_size,
    metric_hbm, curvature_hbm, conserved_hbm, mask_hbm,
    plain, curv, rhs, held, slope, step_out,
    met, flu, inv, mask,
    pack_up, pack_down, from_low, from_high,
    own, got_1, got_2, got_3,
    local_sem, halo_sem, max_send, max_recv, token_y, token_z,
):
    gx, gy, gz = lax.axis_index("gx"), lax.axis_index("gy"), lax.axis_index("gz")
    x, y_lo = lax.rem(gy, X), gy // X
    core, y_hi = lax.rem(gz, CORES), gz // CORES
    y = y_hi * Y_LO + y_lo
    gy_size, gz_size = X * Y_LO, Y_HI * CORES

    load_flu = pltpu.make_async_copy(conserved_hbm, flu.at[:, 1:17, 8:24, :], local_sem.at[0])
    load_mask = pltpu.make_async_copy(mask_hbm, mask, local_sem.at[1])
    load_met = pltpu.make_async_copy(metric_hbm, met.at[:, 3:19, 8:24, :], local_sem.at[2])
    load_curv = pltpu.make_async_copy(curvature_hbm, curv, local_sem.at[3])
    load_flu.start()
    load_mask.start()
    load_plain = pltpu.make_async_copy(metric_hbm, plain, local_sem.at[4])

    group_1 = []
    for dx in far_first(X):
        for dc in range(CORES):
            if dx or dc:
                group_1.append(
                    {"gx": gx, "gy": y_lo * X + lax.rem(x + dx, X), "gz": y_hi * CORES + lax.rem(core + dc, CORES)}
                )
    group_2 = []
    for dy in far_first(Y)[:-1]:
        there = lax.rem(y + dy, Y)
        group_2.append({"gx": gx, "gy": lax.rem(there, Y_LO) * X + x, "gz": (there // Y_LO) * CORES + core})
    before = lax.rem(y + Y - 1, Y)
    y_before = {"gx": gx, "gy": lax.rem(before, Y_LO) * X + x, "gz": (before // Y_LO) * CORES + core}
    group_3 = [{"gx": lax.rem(gx + dz, gx_size), "gy": gy, "gz": gz} for dz in far_first(gx_size)[:-1]]
    x_up = {"gx": lax.rem(gx + 1, gx_size), "gy": gy, "gz": gz}
    x_down = {"gx": lax.rem(gx + gx_size - 1, gx_size), "gy": gy, "gz": gz}
    y_up = {"gx": gx, "gy": lax.rem(gy + 1, gy_size), "gz": gz}
    y_down = {"gx": gx, "gy": lax.rem(gy + gy_size - 1, gy_size), "gz": gz}
    z_up = {"gx": gx, "gy": gy, "gz": lax.rem(gz + 1, gz_size)}
    z_down = {"gx": gx, "gy": gy, "gz": lax.rem(gz + gz_size - 1, gz_size)}

    near_y = group_2[1:]
    z_at = lambda d: {"gx": lax.rem(gx + gx_size + d, gx_size), "gy": gy, "gz": gz}
    barrier = pltpu.get_barrier_semaphore()
    greeted = group_1 + near_y + [z_at(1), z_at(-1), y_up, y_down, z_up, z_down]
    for peer in greeted:
        pl.semaphore_signal(barrier, inc=1, device_id=peer, device_id_type=MESH)

    load_flu.wait()
    load_mask.wait()
    load_met.start()
    load_plain.start()
    load_curv.start()
    lane = lax.broadcasted_iota(jnp.int32, (16, 128), 1)
    block = lane // MB
    matter = jnp.zeros((16, 128), jnp.int32)
    for b in range(128 // MB):
        matter = jnp.where(block == b, mask[0, 0, b], matter)
    live = matter > 0
    fastest = jnp.full((16, 128), sound_speed, jnp.float32)
    for i in range(16):
        density = flu[0, 1 + i, 8:24, :]
        largest = jnp.abs(flu[1, 1 + i, 8:24, :])
        for d in (2, 3):
            largest = jnp.maximum(largest, jnp.abs(flu[d, 1 + i, 8:24, :]))
        fastest = jnp.maximum(fastest, jnp.where(live, largest / density + sound_speed, sound_speed))
    own[0] = jnp.max(fastest, axis=0, keepdims=True)

    pl.semaphore_wait(barrier, len(greeted))

    sends = []

    def spread(stage, group, got):
        copies = []
        for slot, peer in enumerate(group):
            copy = pltpu.make_async_remote_copy(
                src_ref=own.at[stage],
                dst_ref=got.at[slot],
                send_sem=max_send,
                recv_sem=max_recv.at[stage],
                device_id=peer,
                device_id_type=MESH,
            )
            copy.start()
            copies.append(copy)
        sends.extend(copies)
        return len(copies)

    def arrive(ref, sem):
        pltpu.make_async_copy(ref, ref, sem).wait()

    def gather(count, stage, got):
        arrive(got, max_recv.at[stage])
        best = own[stage]
        for slot in range(count):
            best = jnp.maximum(best, got[slot])
        return best

    def tell(token, peer):
        pl.semaphore_signal(token, inc=1, device_id=peer, device_id_type=MESH)

    stage_1 = spread(0, group_1, got_1)
    tell(token_y, y_before)
    for d in (1, -1):
        tell(token_z.at[0], z_at(d))

    halos = []

    def send_halo(src, dst, peer):
        copy = pltpu.make_async_remote_copy(
            src_ref=src,
            dst_ref=dst,
            send_sem=halo_sem.at[0],
            recv_sem=halo_sem.at[1],
            device_id=peer,
            device_id_type=MESH,
        )
        copy.start()
        halos.append(copy)

    send_halo(flu.at[:, 16:17, 8:24, :], flu.at[:, 0:1, 8:24, :], x_up)
    send_halo(flu.at[:, 1:2, 8:24, :], flu.at[:, 17:18, 8:24, :], x_down)
    send_halo(flu.at[:, 1:17, 23:24, :], flu.at[:, 1:17, 7:8, :], y_up)
    send_halo(flu.at[:, 1:17, 8:9, :], flu.at[:, 1:17, 24:25, :], y_down)
    load_met.wait()
    send_halo(met.at[:, 16:19, 8:24, :], met.at[:, 0:3, 8:24, :], x_up)
    send_halo(met.at[:, 3:6, 8:24, :], met.at[:, 19:22, 8:24, :], x_down)
    send_halo(met.at[:, 3:19, 21:24, :], met.at[:, 3:19, 5:8, :], y_up)
    send_halo(met.at[:, 3:19, 8:11, :], met.at[:, 3:19, 24:27, :], y_down)

    group_of = lane // 4
    for f in range(5):
        up = jnp.zeros((16, 128), jnp.float32)
        down = jnp.zeros((16, 128), jnp.float32)
        for half in range(2):
            c = 2 * f + half
            for i in range(16):
                k = half * 16 + i
                plane = met[c, 3 + i, 8:24, :] if c < 6 else flu[c - 6, 1 + i, 8:24, :]
                up = jnp.where(group_of == k, pltpu.roll(plane, (4 * k + 4) % 128, 1), up)
                down = jnp.where(group_of == k, pltpu.roll(plane, 4 * k, 1) if k else plane, down)
        pack_up[f] = up
        pack_down[f] = down
    send_halo(pack_up, from_low, z_up)
    send_halo(pack_down, from_high, z_down)

    pl.semaphore_wait(token_z.at[0], 2)
    for d in (2, -2):
        tell(token_z.at[1], z_at(d))
    pl.semaphore_wait(token_y, 1)

    own[1] = gather(stage_1, 0, got_1)
    stage_2 = spread(1, group_2, got_2)
    pl.semaphore_wait(token_z.at[1], 2)
    for d in (2, -2):
        tell(token_z.at[2], z_at(d))
    own[2] = gather(stage_2, 1, got_2)
    pl.semaphore_wait(token_z.at[2], 2)
    stage_3 = spread(2, group_3, got_3)

    all_halos = met.at[0:4, 0:14, 0:28, :]
    arrive(all_halos, halo_sem.at[1])

    for i in range(18):
        inv[i, 0:32, :] = 1.0 / flu[0, i, 0:32, :]

    def plane_step(i, carry):
        def z_halo(c):
            k = (c % 2) * 16 + i
            low = pltpu.roll(from_low[c // 2], lax.rem(124 - 4 * k + 128, 128), 1)
            high = pltpu.roll(from_high[c // 2], lax.rem(128 - 4 * k, 128), 1)
            return low, high

        def along_z(value, low, high, offset):
            if offset > 0:
                return pltpu.roll(jnp.where(lane < offset, high, value), 128 - offset, 1)
            return pltpu.roll(jnp.where(lane >= 128 + offset, low, value), -offset, 1)

        density = flu[0, 1 + i, 8:24, :]
        inverse = inv[1 + i, 8:24, :]
        moment = [flu[1 + d, 1 + i, 8:24, :] for d in range(3)]
        velocity = [m * inverse for m in moment]

        potential = {}
        for c in range(6):
            low, high = z_halo(c)
            value = met[c, 3 + i, 8:24, :]
            laplacian = (3.0 * second_stencil[3]) * value
            for n in range(3):
                o = 3 - n
                pairs = (
                    (met[c, 3 + i + o, 8:24, :], met[c, 3 + i - o, 8:24, :]),
                    (met[c, 3 + i, 8 + o : 24 + o, :], met[c, 3 + i, 8 - o : 24 - o, :]),
                    (along_z(value, low, high, o), along_z(value, low, high, -o)),
                )
                total = None
                for d, (above, below) in enumerate(pairs):
                    both = above + below
                    total = both if total is None else total + both
                    if c in diagonal:
                        change = above - below
                        key = (d, n)
                        potential[key] = change if key not in potential else potential[key] + change
                laplacian = laplacian + second_stencil[n] * total
            a, b = pair_first[c], pair_second[c]
            stress = moment[a] * velocity[b]
            if a == b:
                stress = stress + sound_square * density
            rhs[c, i] = eight_pi * stress - 0.5 * laplacian

        def cell(dim, offset):
            if dim == 0:
                state = [flu[c, 1 + i + offset, 8:24, :] for c in range(4)]
                inverse_there = inv[1 + i + offset, 8:24, :]
            elif dim == 1:
                state = [flu[c, 1 + i, 8 + offset : 24 + offset, :] for c in range(4)]
                inverse_there = inv[1 + i, 8 + offset : 24 + offset, :]
            else:
                state = []
                for c in range(4):
                    low, high = z_halo(6 + c)
                    here = density if c == 0 else moment[c - 1]
                    state.append(along_z(here, low, high, offset))
                inverse_there = 1.0 / state[0]
            speed_there = state[1 + dim] * inverse_there
            flux = [state[1 + dim]]
            for d in range(3):
                term = state[1 + d] * speed_there
                if d == dim:
                    term = term + sound_square * state[0]
                flux.append(term)
            return state, flux

        around = [None] * 4
        outflow = [None] * 4
        for dim in range(3):
            state_up, flux_up = cell(dim, 1)
            state_down, flux_down = cell(dim, -1)
            for c in range(4):
                both = state_up[c] + state_down[c]
                net = flux_up[c] - flux_down[c]
                around[c] = both if around[c] is None else around[c] + both
                outflow[c] = net if outflow[c] is None else outflow[c] + net
        here = [density] + moment
        for c in range(4):
            kept = here[c] + (0.5 * courant) * (around[c] - 6.0 * here[c])
            rate = -0.5 * outflow[c]
            if c > 0:
                gradient = None
                for n in range(3):
                    term = (-0.5 * first_stencil[n]) * potential[(c - 1, n)]
                    gradient = term if gradient is None else gradient + term
                rate = rate + density * gradient
            held[c, i] = jnp.where(live, kept, here[c])
            slope[c, i] = jnp.where(live, rate, 0.0)
        return carry

    lax.fori_loop(0, 16, plane_step, 0)

    load_curv.wait()
    load_plain.wait()
    best = gather(stage_3, 2, got_3)
    speed_max = jnp.max(best, axis=1, keepdims=True)
    step_out[...] = jnp.broadcast_to(courant / speed_max, (16, 128))

    arrive(all_halos, halo_sem.at[0])
    arrive(met.at[0, 0:1, 0 : len(sends), :], max_send)


def advance(plain, curv, rhs, held, slope, step_in, metric_hbm, curvature_hbm, conserved_hbm, met, bent, flu, sem):
    step = step_in[...]
    copies = []

    def put(src, dst, at):
        copy = pltpu.make_async_copy(src.at[at], dst.at[at], sem.at[len(copies)])
        copy.start()
        copies.append(copy)

    for c in range(4):
        for i in range(16):
            flu[c, i] = held[c, i] + step * slope[c, i]
        put(flu, conserved_hbm, c)
    for c in range(6):
        for i in range(16):
            bend = curv[c, i]
            met[c, i] = plain[c, i] - (2.0 * step) * bend
            bent[c, i] = bend + step * rhs[c, i]
        put(met, metric_hbm, c)
        put(bent, curvature_hbm, c)
    for copy in copies:
        copy.wait()


def body(gx_size, metric, curvature, conserved, matter_mask):
    f32 = jnp.float32
    sym, fluid = metric.shape, conserved.shape
    anywhere = pl.BlockSpec(memory_space=pl.ANY)
    vmem = pl.BlockSpec(memory_space=pltpu.VMEM)
    in_hbm = lambda a: pltpu.with_memory_space_constraint(a, pltpu.HBM)
    in_vmem = lambda a: pltpu.with_memory_space_constraint(a, pltpu.VMEM)
    parts = pl.pallas_call(
        lambda *refs: kernel(gx_size, *refs),
        out_shape=tuple(pltpu.VMEM(s, f32) for s in (sym, sym, sym, fluid, fluid, (16, 128))),
        in_specs=[anywhere] * 4,
        out_specs=(vmem,) * 6,
        scratch_shapes=[
            pltpu.VMEM((6, 22, PITCH, 128), f32),
            pltpu.VMEM((4, 18, PITCH, 128), f32),
            pltpu.VMEM((18, PITCH, 128), f32),
            pltpu.SMEM(matter_mask.shape, jnp.int32),
            pltpu.VMEM((5, 16, 128), f32),
            pltpu.VMEM((5, 16, 128), f32),
            pltpu.VMEM((5, 16, 128), f32),
            pltpu.VMEM((5, 16, 128), f32),
            pltpu.VMEM((3, 1, 128), f32),
            pltpu.VMEM((X * CORES - 1, 1, 128), f32),
            pltpu.VMEM((Y - 1, 1, 128), f32),
            pltpu.VMEM((gx_size - 1, 1, 128), f32),
            pltpu.SemaphoreType.DMA((5,)),
            pltpu.SemaphoreType.DMA((2,)),
            pltpu.SemaphoreType.DMA,
            pltpu.SemaphoreType.DMA((3,)),
            pltpu.SemaphoreType.REGULAR,
            pltpu.SemaphoreType.REGULAR((3,)),
        ],
        compiler_params=pltpu.CompilerParams(
            collective_id=0, has_side_effects=True, vmem_limit_bytes=24 * 1024 * 1024
        ),
        name="exchange",
    )(in_hbm(metric), in_hbm(curvature), in_hbm(conserved), in_hbm(matter_mask))
    return pl.pallas_call(
        advance,
        out_shape=tuple(jax.ShapeDtypeStruct(s, f32) for s in (sym, sym, fluid)),
        in_specs=[vmem] * 6,
        out_specs=(anywhere,) * 3,
        scratch_shapes=[
            pltpu.VMEM(sym, f32),
            pltpu.VMEM(sym, f32),
            pltpu.VMEM(fluid, f32),
            pltpu.SemaphoreType.DMA((16,)),
        ],
        compiler_params=pltpu.CompilerParams(vmem_limit_bytes=16 * 1024 * 1024),
        name="advance",
    )(*(in_vmem(a) for a in parts))


def solution(mesh):
    cells = P(None, "gx", "gy", "gz")
    return jax.shard_map(
        lambda *args: body(mesh.shape["gx"], *args),
        mesh=mesh,
        in_specs=(cells, cells, cells, P("gx", "gy", "gz")),
        out_specs=(cells, cells, cells),
        check_vma=False,
    )
```

```python
import math

import jax
import jax.numpy as jnp
from jax import lax
from jax.experimental import pallas as pl
from jax.experimental.pallas import tpu as pltpu
from jax.sharding import PartitionSpec as P

MESH = pl.DeviceIdType.MESH
MB = 16
second_stencil = (1.0 / 90.0, -3.0 / 20.0, 1.5, -49.0 / 18.0)
first_stencil = (-1.0 / 60.0, 3.0 / 20.0, -0.75)
sound_square = 0.25
sound_speed = 0.5
courant = 0.3
eight_pi = 8.0 * math.pi
pair_first = (0, 0, 0, 1, 1, 2)
pair_second = (0, 1, 2, 1, 2, 2)
diagonal = (0, 3, 5)

PITCH = 40

EARLY = 3

X, Y_LO, Y_HI, CORES = 4, 2, 4, 2
Y = Y_LO * Y_HI


def far_first(n):
    return sorted(range(n), key=lambda d: -min(d, n - d))


def kernel(
    gx_size,
    metric_hbm, curvature_hbm, conserved_hbm, mask_hbm,
    plain, curv, rhs, held, slope, step_out,
    met, flu, inv, mask,
    pack_up, pack_down, from_low, from_high,
    own, got_1, got_2, got_3,
    local_sem, halo_sem, max_send, max_recv, token_y, token_z,
):
    gx, gy, gz = lax.axis_index("gx"), lax.axis_index("gy"), lax.axis_index("gz")
    x, y_lo = lax.rem(gy, X), gy // X
    core, y_hi = lax.rem(gz, CORES), gz // CORES
    y = y_hi * Y_LO + y_lo
    gy_size, gz_size = X * Y_LO, Y_HI * CORES
    early = gx < EARLY

    load_flu = pltpu.make_async_copy(conserved_hbm, flu.at[:, 1:17, 8:24, :], local_sem.at[0])
    load_mask = pltpu.make_async_copy(mask_hbm, mask, local_sem.at[1])
    load_met = pltpu.make_async_copy(metric_hbm, met.at[:, 3:19, 8:24, :], local_sem.at[2])
    load_curv = pltpu.make_async_copy(curvature_hbm, curv, local_sem.at[3])
    load_flu.start()
    load_mask.start()
    load_plain = pltpu.make_async_copy(metric_hbm, plain, local_sem.at[4])

    group_1 = []
    for dx in far_first(X):
        for dc in range(CORES):
            if dx or dc:
                group_1.append(
                    {"gx": gx, "gy": y_lo * X + lax.rem(x + dx, X), "gz": y_hi * CORES + lax.rem(core + dc, CORES)}
                )
    group_2 = []
    for dy in far_first(Y)[:-1]:
        there = lax.rem(y + dy, Y)
        group_2.append({"gx": gx, "gy": lax.rem(there, Y_LO) * X + x, "gz": (there // Y_LO) * CORES + core})
    before = lax.rem(y + Y - 1, Y)
    y_before = {"gx": gx, "gy": lax.rem(before, Y_LO) * X + x, "gz": (before // Y_LO) * CORES + core}
    group_3 = [{"gx": lax.rem(gx + dz, gx_size), "gy": gy, "gz": gz} for dz in far_first(gx_size)[:-1]]
    x_up = {"gx": lax.rem(gx + 1, gx_size), "gy": gy, "gz": gz}
    x_down = {"gx": lax.rem(gx + gx_size - 1, gx_size), "gy": gy, "gz": gz}
    y_up = {"gx": gx, "gy": lax.rem(gy + 1, gy_size), "gz": gz}
    y_down = {"gx": gx, "gy": lax.rem(gy + gy_size - 1, gy_size), "gz": gz}
    z_up = {"gx": gx, "gy": gy, "gz": lax.rem(gz + 1, gz_size)}
    z_down = {"gx": gx, "gy": gy, "gz": lax.rem(gz + gz_size - 1, gz_size)}

    near_y = group_2[1:]
    z_at = lambda d: {"gx": lax.rem(gx + gx_size + d, gx_size), "gy": gy, "gz": gz}
    barrier = pltpu.get_barrier_semaphore()
    greeted = group_1 + near_y + [z_at(1), z_at(-1), y_up, y_down, z_up, z_down]
    for peer in greeted:
        pl.semaphore_signal(barrier, inc=1, device_id=peer, device_id_type=MESH)

    load_flu.wait()
    load_mask.wait()
    load_met.start()
    load_plain.start()
    load_curv.start()
    lane = lax.broadcasted_iota(jnp.int32, (16, 128), 1)
    block = lane // MB
    matter = jnp.zeros((16, 128), jnp.int32)
    for b in range(128 // MB):
        matter = jnp.where(block == b, mask[0, 0, b], matter)
    live = matter > 0
    fastest = jnp.full((16, 128), sound_speed, jnp.float32)
    for i in range(16):
        density = flu[0, 1 + i, 8:24, :]
        largest = jnp.abs(flu[1, 1 + i, 8:24, :])
        for d in (2, 3):
            largest = jnp.maximum(largest, jnp.abs(flu[d, 1 + i, 8:24, :]))
        fastest = jnp.maximum(fastest, jnp.where(live, largest / density + sound_speed, sound_speed))
    own[0] = jnp.max(fastest, axis=0, keepdims=True)

    pl.semaphore_wait(barrier, len(greeted))

    def spread(stage, group, got):
        for slot, peer in enumerate(group):
            copy = pltpu.make_async_remote_copy(
                src_ref=own.at[stage],
                dst_ref=got.at[slot],
                send_sem=max_send,
                recv_sem=max_recv.at[stage],
                device_id=peer,
                device_id_type=MESH,
            )
            copy.start()

    def arrive(ref, sem):
        pltpu.make_async_copy(ref, ref, sem).wait()

    def gather(count, stage, got):
        arrive(got, max_recv.at[stage])
        best = own[stage]
        for slot in range(count):
            best = jnp.maximum(best, got[slot])
        return best

    def tell(token, peer):
        pl.semaphore_signal(token, inc=1, device_id=peer, device_id_type=MESH)

    spread(0, group_1, got_1)
    tell(token_y, y_before)
    for d in (1, -1):
        tell(token_z.at[0], z_at(d))

    def send_halo(src, dst, peer):
        copy = pltpu.make_async_remote_copy(
            src_ref=src,
            dst_ref=dst,
            send_sem=halo_sem.at[0],
            recv_sem=halo_sem.at[1],
            device_id=peer,
            device_id_type=MESH,
        )
        copy.start()

    def send_y():
        send_halo(flu.at[:, 1:17, 23:24, :], flu.at[:, 1:17, 7:8, :], y_up)
        send_halo(flu.at[:, 1:17, 8:9, :], flu.at[:, 1:17, 24:25, :], y_down)
        send_halo(met.at[:, 3:19, 21:24, :], met.at[:, 3:19, 5:8, :], y_up)
        send_halo(met.at[:, 3:19, 8:11, :], met.at[:, 3:19, 24:27, :], y_down)

    load_met.wait()
    pl.when(early)(send_y)
    send_halo(flu.at[:, 16:17, 8:24, :], flu.at[:, 0:1, 8:24, :], x_up)
    send_halo(flu.at[:, 1:2, 8:24, :], flu.at[:, 17:18, 8:24, :], x_down)
    send_halo(met.at[:, 16:19, 8:24, :], met.at[:, 0:3, 8:24, :], x_up)
    send_halo(met.at[:, 3:6, 8:24, :], met.at[:, 19:22, 8:24, :], x_down)

    group_of = lane // 4
    for f in range(5):
        up = jnp.zeros((16, 128), jnp.float32)
        down = jnp.zeros((16, 128), jnp.float32)
        for half in range(2):
            c = 2 * f + half
            for i in range(16):
                k = half * 16 + i
                plane = met[c, 3 + i, 8:24, :] if c < 6 else flu[c - 6, 1 + i, 8:24, :]
                up = jnp.where(group_of == k, pltpu.roll(plane, (4 * k + 4) % 128, 1), up)
                down = jnp.where(group_of == k, pltpu.roll(plane, 4 * k, 1) if k else plane, down)
        pack_up[f] = up
        pack_down[f] = down
    send_halo(pack_up, from_low, z_up)
    send_halo(pack_down, from_high, z_down)

    pl.semaphore_wait(token_z.at[0], 2)
    for d in (2, -2):
        tell(token_z.at[1], z_at(d))
    pl.semaphore_wait(token_y, 1)

    own[1] = gather(len(group_1), 0, got_1)
    spread(1, group_2, got_2)
    pl.when(jnp.logical_not(early))(send_y)
    pl.semaphore_wait(token_z.at[1], 2)
    for d in (2, -2):
        tell(token_z.at[2], z_at(d))

    def pass_on():
        own[2] = gather(len(group_2), 1, got_2)
        pl.semaphore_wait(token_z.at[2], 2)
        spread(2, group_3, got_3)

    pl.when(jnp.logical_not(early))(pass_on)

    all_halos = met.at[0:4, 0:14, 0:28, :]
    arrive(all_halos, halo_sem.at[1])

    for i in range(18):
        inv[i, 0:32, :] = 1.0 / flu[0, i, 0:32, :]

    def plane_step(i, carry):
        def z_halo(c):
            k = (c % 2) * 16 + i
            low = pltpu.roll(from_low[c // 2], lax.rem(124 - 4 * k + 128, 128), 1)
            high = pltpu.roll(from_high[c // 2], lax.rem(128 - 4 * k, 128), 1)
            return low, high

        def along_z(value, low, high, offset):
            if offset > 0:
                return pltpu.roll(jnp.where(lane < offset, high, value), 128 - offset, 1)
            return pltpu.roll(jnp.where(lane >= 128 + offset, low, value), -offset, 1)

        density = flu[0, 1 + i, 8:24, :]
        inverse = inv[1 + i, 8:24, :]
        moment = [flu[1 + d, 1 + i, 8:24, :] for d in range(3)]
        velocity = [m * inverse for m in moment]

        potential = {}
        for c in range(6):
            low, high = z_halo(c)
            value = met[c, 3 + i, 8:24, :]
            laplacian = (3.0 * second_stencil[3]) * value
            for n in range(3):
                o = 3 - n
                pairs = (
                    (met[c, 3 + i + o, 8:24, :], met[c, 3 + i - o, 8:24, :]),
                    (met[c, 3 + i, 8 + o : 24 + o, :], met[c, 3 + i, 8 - o : 24 - o, :]),
                    (along_z(value, low, high, o), along_z(value, low, high, -o)),
                )
                total = None
                for d, (above, below) in enumerate(pairs):
                    both = above + below
                    total = both if total is None else total + both
                    if c in diagonal:
                        change = above - below
                        key = (d, n)
                        potential[key] = change if key not in potential else potential[key] + change
                laplacian = laplacian + second_stencil[n] * total
            a, b = pair_first[c], pair_second[c]
            stress = moment[a] * velocity[b]
            if a == b:
                stress = stress + sound_square * density
            rhs[c, i] = eight_pi * stress - 0.5 * laplacian

        def cell(dim, offset):
            if dim == 0:
                state = [flu[c, 1 + i + offset, 8:24, :] for c in range(4)]
                inverse_there = inv[1 + i + offset, 8:24, :]
            elif dim == 1:
                state = [flu[c, 1 + i, 8 + offset : 24 + offset, :] for c in range(4)]
                inverse_there = inv[1 + i, 8 + offset : 24 + offset, :]
            else:
                state = []
                for c in range(4):
                    low, high = z_halo(6 + c)
                    here = density if c == 0 else moment[c - 1]
                    state.append(along_z(here, low, high, offset))
                inverse_there = 1.0 / state[0]
            speed_there = state[1 + dim] * inverse_there
            flux = [state[1 + dim]]
            for d in range(3):
                term = state[1 + d] * speed_there
                if d == dim:
                    term = term + sound_square * state[0]
                flux.append(term)
            return state, flux

        around = [None] * 4
        outflow = [None] * 4
        for dim in range(3):
            state_up, flux_up = cell(dim, 1)
            state_down, flux_down = cell(dim, -1)
            for c in range(4):
                both = state_up[c] + state_down[c]
                net = flux_up[c] - flux_down[c]
                around[c] = both if around[c] is None else around[c] + both
                outflow[c] = net if outflow[c] is None else outflow[c] + net
        here = [density] + moment
        for c in range(4):
            kept = here[c] + (0.5 * courant) * (around[c] - 6.0 * here[c])
            rate = -0.5 * outflow[c]
            if c > 0:
                gradient = None
                for n in range(3):
                    term = (-0.5 * first_stencil[n]) * potential[(c - 1, n)]
                    gradient = term if gradient is None else gradient + term
                rate = rate + density * gradient
            held[c, i] = jnp.where(live, kept, here[c])
            slope[c, i] = jnp.where(live, rate, 0.0)
        return carry

    lax.fori_loop(0, 16, plane_step, 0)
    pl.when(early)(pass_on)

    load_curv.wait()
    load_plain.wait()
    best = gather(len(group_3), 2, got_3)
    speed_max = jnp.max(best, axis=1, keepdims=True)
    step_out[...] = jnp.broadcast_to(courant / speed_max, (16, 128))

    arrive(all_halos, halo_sem.at[0])
    arrive(met.at[0, 0:1, 0 : len(group_1 + group_2 + group_3), :], max_send)


def advance(plain, curv, rhs, held, slope, step_in, metric_hbm, curvature_hbm, conserved_hbm, met, bent, flu, sem):
    step = step_in[...]
    copies = []

    def put(src, dst, at):
        copy = pltpu.make_async_copy(src.at[at], dst.at[at], sem.at[len(copies)])
        copy.start()
        copies.append(copy)

    for c in range(4):
        for i in range(16):
            flu[c, i] = held[c, i] + step * slope[c, i]
        put(flu, conserved_hbm, c)
    for c in range(6):
        for i in range(16):
            bend = curv[c, i]
            met[c, i] = plain[c, i] - (2.0 * step) * bend
            bent[c, i] = bend + step * rhs[c, i]
        put(met, metric_hbm, c)
        put(bent, curvature_hbm, c)
    for copy in copies:
        copy.wait()


def body(gx_size, metric, curvature, conserved, matter_mask):
    f32 = jnp.float32
    sym, fluid = metric.shape, conserved.shape
    anywhere = pl.BlockSpec(memory_space=pl.ANY)
    vmem = pl.BlockSpec(memory_space=pltpu.VMEM)
    in_hbm = lambda a: pltpu.with_memory_space_constraint(a, pltpu.HBM)
    in_vmem = lambda a: pltpu.with_memory_space_constraint(a, pltpu.VMEM)
    parts = pl.pallas_call(
        lambda *refs: kernel(gx_size, *refs),
        out_shape=tuple(pltpu.VMEM(s, f32) for s in (sym, sym, sym, fluid, fluid, (16, 128))),
        in_specs=[anywhere] * 4,
        out_specs=(vmem,) * 6,
        scratch_shapes=[
            pltpu.VMEM((6, 22, PITCH, 128), f32),
            pltpu.VMEM((4, 18, PITCH, 128), f32),
            pltpu.VMEM((18, PITCH, 128), f32),
            pltpu.SMEM(matter_mask.shape, jnp.int32),
            pltpu.VMEM((5, 16, 128), f32),
            pltpu.VMEM((5, 16, 128), f32),
            pltpu.VMEM((5, 16, 128), f32),
            pltpu.VMEM((5, 16, 128), f32),
            pltpu.VMEM((3, 1, 128), f32),
            pltpu.VMEM((X * CORES - 1, 1, 128), f32),
            pltpu.VMEM((Y - 1, 1, 128), f32),
            pltpu.VMEM((gx_size - 1, 1, 128), f32),
            pltpu.SemaphoreType.DMA((5,)),
            pltpu.SemaphoreType.DMA((2,)),
            pltpu.SemaphoreType.DMA,
            pltpu.SemaphoreType.DMA((3,)),
            pltpu.SemaphoreType.REGULAR,
            pltpu.SemaphoreType.REGULAR((3,)),
        ],
        compiler_params=pltpu.CompilerParams(
            collective_id=0, has_side_effects=True, vmem_limit_bytes=24 * 1024 * 1024
        ),
        name="exchange",
    )(in_hbm(metric), in_hbm(curvature), in_hbm(conserved), in_hbm(matter_mask))
    return pl.pallas_call(
        advance,
        out_shape=tuple(jax.ShapeDtypeStruct(s, f32) for s in (sym, sym, fluid)),
        in_specs=[vmem] * 6,
        out_specs=(anywhere,) * 3,
        scratch_shapes=[
            pltpu.VMEM(sym, f32),
            pltpu.VMEM(sym, f32),
            pltpu.VMEM(fluid, f32),
            pltpu.SemaphoreType.DMA((16,)),
        ],
        compiler_params=pltpu.CompilerParams(vmem_limit_bytes=16 * 1024 * 1024),
        name="advance",
    )(*(in_vmem(a) for a in parts))


def solution(mesh):
    cells = P(None, "gx", "gy", "gz")
    return jax.shard_map(
        lambda *args: body(mesh.shape["gx"], *args),
        mesh=mesh,
        in_specs=(cells, cells, cells, P("gx", "gy", "gz")),
        out_specs=(cells, cells, cells),
        check_vma=False,
    )
```
